256 devices in a mesh: depth: 2 (over x_hi), tx: 16 (over z, core), ty: 8 (over x_lo, y).
Axes of the slice: x: 4 (x_hi: 2, x_lo: 2; x = x_hi * 2 + x_lo), y: 4, z: 8, core: 2. Of those that a mesh axis runs over, the one named last changes fastest.
Arguments:
- down_state: float32 [2, 8, 2, 2, 512, 1024], P('depth', None, None, None, 'tx', 'ty'), may hold values from -6 to 6
- up_state: float32 [2, 8, 2, 2, 512, 1024], P('depth', None, None, None, 'tx', 'ty'), may hold values from -6 to 6
- incident: float32 [8, 2, 2, 512, 1024], P(None, None, None, 'tx', 'ty'), may hold values from -6 to 6
- medium_map: int32 [2, 512, 1024], P('depth', 'tx', 'ty'), may hold values from 0 to 15
- media_table: float32 [16, 16], replicated, may hold values from -0.3 to 0.3
- tap_index: int32 [2, 2], P('depth'), may hold values from 0 to 7, as said below
- kernel_bank: float32 [8, 2, 33], replicated, may hold values from -0.7 to 0.7
Outputs:
- down_final: float32 [2, 8, 2, 2, 512, 1024], P('depth', None, None, None, 'tx', 'ty')
- up_final: float32 [2, 8, 2, 2, 512, 1024], P('depth', None, None, None, 'tx', 'ty')
The draws below stay inside these ranges and needn't reach their ends.
Inputs may be any that keep to these rules, and one draw needn't show every extreme that they name: `tap_index`: all entries are distinct; 0 and 7 both occur.
All inputs are finite; a program needn't handle non-finite values.
Results may differ from the reference program's by a relative error of at most 0.00011.
Values sent between devices are 32-bit elements; how exact they have to be, the bound alone decides.
No kernel may reach another device: no remote copies, remote signals or barrier semaphores. Data moves between devices by JAX's collectives and lax.ppermute only.
A program may use at most 64 MiB of HBM per device.

```python
import jax
import jax.numpy as jnp
from jax import lax

ILLUM = 8
POL = 2
TAPS = 33
TICKS = 4
MEDIA = 16
KERNELS = 8
NX = 512
NY = 1024
SECTIONS = 2


def draw_tap_index(key, part):
    count = SECTIONS * 2
    middle = 1 + jax.random.permutation(jax.random.fold_in(key, 7), KERNELS - 2)[:count - 2].astype(jnp.int32)
    chosen = jnp.concatenate([jnp.array([0, KERNELS - 1], dtype=jnp.int32), middle])
    shuffled = jax.random.permutation(jax.random.fold_in(key, 11), chosen)
    return shuffled.reshape((SECTIONS, 2)).astype(jnp.int32)


def touch_ends(result, own_key, low, high):
    extent = result.shape
    place = [jax.random.randint(jax.random.fold_in(own_key, axis), (), 0, extent[axis]) for axis in range(len(extent))]
    result = result.at[tuple(place)].set(low)
    longest = extent.index(max(extent))
    place[longest] = (place[longest] + 1) % extent[longest]
    return result.at[tuple(place)].set(high)


def shard_levels(own_key, extent, cuts, least, high):
    def one(position, parts):
        steps = jax.random.uniform(jax.random.fold_in(jax.random.fold_in(own_key, 6), position), (parts,), jnp.float32, least / len(cuts), high / len(cuts))
        return jnp.repeat(jnp.exp(steps), extent[position] // parts).reshape((-1,) + (1,) * (len(extent) - position - 1))

    gain = one(*cuts[0])
    for cut in cuts[1:]:
        gain = gain * one(*cut)
    return gain


def normal_values(own_key, dims, spread, limit, split=(), kind=jnp.bfloat16):
    level = shard_levels(own_key, dims, split, -0.22, 0.18) if split else 1.0
    values = jax.random.normal(own_key, dims, jnp.float32) * spread * level
    return jnp.minimum(jnp.maximum(values, -limit), limit).astype(kind)


def setup_inputs(seed: int = 0) -> dict:
    arg_keys = jax.random.split(jax.random.key(seed), 8)
    return {
        "down_state": normal_values(arg_keys[0], (SECTIONS, ILLUM, 2, POL, NX, NY), 1.0, 6.0, ((0, 2), (4, 16), (5, 8)), jnp.float32),
        "up_state": normal_values(arg_keys[1], (SECTIONS, ILLUM, 2, POL, NX, NY), 1.0, 6.0, ((0, 2), (4, 16), (5, 8)), jnp.float32),
        "incident": normal_values(arg_keys[2], (ILLUM, 2, POL, NX, NY), 1.0, 6.0, ((3, 16), (4, 8)), jnp.float32),
        "medium_map": touch_ends(jax.random.randint(arg_keys[3], (SECTIONS, NX, NY), 0, MEDIA), jax.random.fold_in(arg_keys[3], 1), 0, MEDIA - 1).astype(jnp.int32),
        "media_table": jnp.clip(jax.random.uniform(arg_keys[4], (MEDIA, 16), jnp.float32, -0.3, 0.3), -0.3, 0.3),
        "tap_index": draw_tap_index(jax.random.fold_in(arg_keys[7], 71), 0),
        "kernel_bank": normal_values(arg_keys[6], (KERNELS, 2, TAPS), 0.123, 0.7, (), jnp.float32),
    }


def propagate_axis(wavefield, tap_pair, axis_pos):
    halfwidth = tap_pair.shape[-1] // 2
    margins = [(0, 0)] * 5
    margins[axis_pos] = (halfwidth, halfwidth)
    padded = jnp.pad(wavefield, margins)
    length = wavefield.shape[axis_pos]
    real_sum = jnp.zeros_like(wavefield[:, 0])
    imag_sum = jnp.zeros_like(wavefield[:, 0])
    for offset in range(tap_pair.shape[-1]):
        window = lax.slice_in_dim(padded, offset, offset + length, axis=axis_pos)
        real_sum = real_sum + tap_pair[0, offset] * window[:, 0] - tap_pair[1, offset] * window[:, 1]
        imag_sum = imag_sum + tap_pair[0, offset] * window[:, 1] + tap_pair[1, offset] * window[:, 0]
    return jnp.stack([real_sum, imag_sum], axis=1)


def jones_apply(real_mat, imag_mat, wavefield):
    real_in = wavefield[:, 0]
    imag_in = wavefield[:, 1]
    real_out = jnp.sum(real_mat[None] * real_in[:, None], axis=2) - jnp.sum(imag_mat[None] * imag_in[:, None], axis=2)
    imag_out = jnp.sum(real_mat[None] * imag_in[:, None], axis=2) + jnp.sum(imag_mat[None] * real_in[:, None], axis=2)
    return jnp.stack([real_out, imag_out], axis=1)


def scatter_section(down_prop, up_prop, entries):
    shape_tail = entries.shape[1:]
    identity = jnp.eye(2, dtype=jnp.float32)[:, :, None, None]
    trans_real = entries[0:4].reshape((2, 2) + shape_tail) + 0.5 * identity
    trans_imag = entries[4:8].reshape((2, 2) + shape_tail)
    refl_real = entries[8:12].reshape((2, 2) + shape_tail)
    refl_imag = entries[12:16].reshape((2, 2) + shape_tail)
    down_out = jones_apply(trans_real, trans_imag, down_prop) + jones_apply(refl_real, refl_imag, up_prop)
    up_out = jones_apply(trans_real, trans_imag, up_prop) - jones_apply(refl_real, refl_imag, down_prop)
    return down_out, up_out


def reference(down_state, up_state, incident, medium_map, media_table, tap_index, kernel_bank):
    sections = down_state.shape[0]
    downs = [down_state[section] for section in range(sections)]
    ups = [up_state[section] for section in range(sections)]
    for moment in range(TICKS):
        down_outs = []
        up_outs = []
        for section in range(sections):
            kernel_rows = kernel_bank[tap_index[section, 0]]
            kernel_cols = kernel_bank[tap_index[section, 1]]
            down_prop = propagate_axis(propagate_axis(downs[section], kernel_rows, 3), kernel_cols, 4)
            up_prop = propagate_axis(propagate_axis(ups[section], kernel_rows, 3), kernel_cols, 4)
            entries = jnp.moveaxis(media_table[medium_map[section]], -1, 0)
            down_out, up_out = scatter_section(down_prop, up_prop, entries)
            down_outs.append(down_out)
            up_outs.append(up_out)
        downs = [incident] + down_outs[:-1]
        ups = up_outs[1:] + [jnp.zeros_like(incident)]
    return jnp.stack(downs), jnp.stack(ups)
```

```python
import functools

import jax
import jax.numpy as jnp
from jax import lax
from jax.experimental import pallas as pl
from jax.experimental.pallas import tpu as pltpu
from jax.sharding import PartitionSpec as P

f32 = jnp.float32
bf16 = jnp.bfloat16
VM = pltpu.VMEM
UNITS = 8
TICKS = 4
TAPS = 33
HALF = 16
ROWS = 32
COLS = 128


def call(body, outs, ins, flops=0, limit=8):
    return pl.pallas_call(
        body,
        out_shape=[jax.ShapeDtypeStruct(s, d) for s, d in outs],
        in_specs=[pl.BlockSpec(memory_space=m) for m in ins],
        out_specs=[pl.BlockSpec(memory_space=VM)] * len(outs),
        cost_estimate=pl.CostEstimate(flops=flops, bytes_accessed=0, transcendentals=0),
        compiler_params=pltpu.CompilerParams(vmem_limit_bytes=limit * 1024 * 1024),
    )


def split(x):
    hi = x.astype(bf16)
    lo = (x - hi.astype(f32)).astype(bf16)
    return hi, lo


def dot(a, b):
    return jnp.dot(a, b, preferred_element_type=f32)


def halves_body(down, up, inc, top, bot):
    def unit(u, _):
        for n, src in enumerate((down, up, inc)):
            for c in range(2):
                for p in range(2):
                    x = src[u, c, p]
                    top[n * UNITS + u, c, p] = x[0:HALF]
                    bot[n * UNITS + u, c, p] = x[HALF:ROWS]
        return 0

    lax.fori_loop(0, UNITS, unit, 0)


def band(diff, bank, row):
    re = jnp.zeros(diff.shape, f32)
    im = jnp.zeros(diff.shape, f32)
    for k in range(TAPS):
        hit = diff == k
        re = jnp.where(hit, bank[row, k], re)
        im = jnp.where(hit, bank[row + 1, k], im)
    return re, im


def iota(shape, dim):
    return lax.broadcasted_iota(jnp.int32, shape, dim)


def prep_body(tap_own, tap_other, bank, table, map_own, map_other, amat, bhi, blo, trans, refl):
    depth = lax.axis_index("depth")
    tx, ty = lax.axis_index("tx"), lax.axis_index("ty")
    tx_low, tx_high = tx == 0, tx == lax.axis_size("tx") - 1
    ty_low, ty_high = ty == 0, ty == lax.axis_size("ty") - 1
    for s in range(2):
        mine = depth == s
        k_row = jnp.where(mine, tap_own[0, 0], tap_other[0, 0]) * 2
        k_col = jnp.where(mine, tap_own[0, 1], tap_other[0, 1]) * 2
        i, j = iota((64, 128), 0), iota((64, 128), 1)
        jj = j & 63
        re, im = band(jj - (i & 31), bank, k_row)
        quad = (i >> 5) * 2 + (j >> 6)
        a = jnp.where(quad == 1, -im, jnp.where(quad == 2, im, re))
        gone = ((jj < HALF) & tx_low) | ((jj >= 48) & tx_high)
        a = jnp.where(gone, 0.0, a)
        hi, lo = split(a)
        amat[s, 0:64, 0:128] = hi
        amat[s, 0:64, 128:256] = hi
        amat[s, 64:128, 0:128] = lo
        amat[s, 64:128, 128:256] = jnp.zeros_like(lo)

        for part in range(2):
            i, j = iota((64, 128), 1), iota((64, 128), 0) + (HALF + 64 * part)
            re, im = band(j - i, bank, k_col)
            (rh, rl), (ih, il) = split(re), split(im)
            for c, (hr, hm, lr, lm) in enumerate(((rh, ih, rl, il), (-ih, rh, -il, rl))):
                rows = pl.ds(c * 128 + 64 * part, 64)
                bhi[s, rows, 0:128] = hr
                bhi[s, rows, 128:256] = hm
                blo[s, rows, 0:128] = lr
                blo[s, rows, 128:256] = lm
        r, i = iota((64, 128), 0), iota((64, 128), 1)
        side = r >> 5
        l = (r & 15) + side * 144
        re, im = band(l - i, bank, k_col)
        gone = ((side == 0) & ty_low) | ((side == 1) & ty_high)
        re, im = jnp.where(gone, 0.0, re), jnp.where(gone, 0.0, im)
        isim = ((r >> 4) & 1) == 1
        one = jnp.where(isim, -im, re)
        two = jnp.where(isim, re, im)
        zero = jnp.zeros((64, 128), bf16)
        for n, v in enumerate((one, two)):
            hi, lo = split(v)
            cols = pl.ds(n * 128, 128)
            bhi[s, 256:320, cols] = hi
            blo[s, 256:320, cols] = lo
            bhi[s, 320:384, cols] = zero
            blo[s, 320:384, cols] = zero

        m = jnp.where(mine, map_own[...], map_other[...])
        hits = [m == e for e in range(16)]
        for q in range(16):
            v = jnp.zeros((ROWS, COLS), f32)
            for e in range(16):
                v = jnp.where(hits[e], table[e, q], v)
            if q < 8:
                if q in (0, 3):
                    v = v + 0.5
                trans[s, q] = v
            else:
                refl[s, q - 8] = v if s == 0 else -v


def section(odd):
    depth = lax.axis_index("depth")
    return 1 - depth if odd else depth


def row_body(groups, odd, amat, top, bot, htop, hbot, w, low, high):
    sec = section(odd)
    lane16 = iota((ROWS, COLS), 1) >> 4

    def group(g, _):
        lhs = amat[jnp.where(g >= 4, 0, sec)]
        packs = [[jnp.zeros((ROWS, COLS), f32) for _ in range(2)] for _ in range(2)]
        for n in range(4):
            u = g * 4 + n
            v = jnp.concatenate(
                [
                    jnp.concatenate([x[u, c, p] for p in range(2)], axis=1)
                    for c in range(2)
                    for x in (htop, top, bot, hbot)
                ],
                axis=0,
            )
            hi, lo = split(v)
            o = dot(lhs, jnp.concatenate([hi, lo], axis=0))
            o = o[0:64] + o[64:128]
            for c in range(2):
                for p in range(2):
                    x = o[c * 32 : c * 32 + 32, p * 128 : p * 128 + 128]
                    w[u, c, p] = x
                    k = n * 2 + c
                    first = pltpu.roll(x, k * 16, 1) if k else x
                    last = pltpu.roll(x, (k * 16 + 16) % 128, 1) if k != 7 else x
                    packs[0][p] = jnp.where(lane16 == k, first, packs[0][p])
                    packs[1][p] = jnp.where(lane16 == k, last, packs[1][p])
        for p in range(2):
            low[g, p] = packs[0][p]
            high[g, p] = packs[1][p]
        return 0

    lax.fori_loop(0, groups, group, 0)


def columns(w, hlow, hhigh, g, bh, bl):
    lane = iota((ROWS, COLS), 1)
    rows = []
    for n in range(4):
        for p in range(2):
            a, b = hlow[g, p], hhigh[g, p]
            a = pltpu.roll(a, 128 - 32 * n, 1) if n else a
            b = pltpu.roll(b, (160 - 32 * n) % 128, 1) if n != 1 else b
            u = g * 4 + n
            rows.append(jnp.concatenate([w[u, 0, p], w[u, 1, p], jnp.where(lane < 32, a, b)], axis=1))
    hi, lo = split(jnp.concatenate(rows, axis=0))
    return dot(hi, bh) + dot(lo, bh) + dot(hi, bl)


def field(o, n):
    return [[o[(n * 2 + p) * 32 : (n * 2 + p) * 32 + 32, c * 128 : c * 128 + 128] for c in range(2)] for p in range(2)]


def jones(m, v):
    out = []
    for q in range(2):
        re = im = None
        for p in range(2):
            a, b = m[q * 2 + p], m[4 + q * 2 + p]
            r = a * v[p][0] - b * v[p][1]
            i = a * v[p][1] + b * v[p][0]
            re, im = (r, i) if re is None else (re + r, im + i)
        out.append((re, im))
    return out


def first_body(bhi, blo, trans, refl, w, hlow, hhigh, top, bot):
    d = section(0)
    bh, bl = bhi[d], blo[d]

    def group(g, _):
        oa = columns(w, hlow, hhigh, d * 2 + g, bh, bl)
        ob = columns(w, hlow, hhigh, (1 - d) * 2 + g, bh, bl)
        for n in range(4):
            a = jones([trans[d, q] for q in range(8)], field(oa, n))
            b = jones([refl[d, q] for q in range(8)], field(ob, n))
            for p in range(2):
                for c in range(2):
                    v = a[p][c] + b[p][c]
                    top[g * 4 + n, c, p] = v[0:16]
                    bot[g * 4 + n, c, p] = v[16:32]
        return 0

    lax.fori_loop(0, UNITS // 4, group, 0)


def inc_body(bhi, blo, trans, w, hlow, hhigh, const):
    bh, bl = bhi[0], blo[0]

    def group(g, _):
        o = columns(w, hlow, hhigh, g + 4, bh, bl)
        for n in range(4):
            a = jones([trans[0, q] for q in range(8)], field(o, n))
            for p in range(2):
                for c in range(2):
                    const[g * 4 + n, c, p] = a[p][c]
        return 0

    lax.fori_loop(0, UNITS // 4, group, 0)


def next_body(last, odd, bhi, blo, refl, const, w, hlow, hhigh, *rest):
    s = section(odd)
    bh, bl = bhi[s], blo[s]
    gate = jnp.where(s == 0, 1.0, 0.0).astype(f32)
    top_section = lax.axis_index("depth") == 0

    def group(g, _):
        o = columns(w, hlow, hhigh, g, bh, bl)
        for n in range(4):
            u = g * 4 + n
            b = jones([refl[s, q] for q in range(8)], field(o, n))
            for p in range(2):
                for c in range(2):
                    v = b[p][c] + gate * const[u, c, p]
                    if last:
                        itop, ibot, down, up = rest
                        i = jnp.concatenate([itop[16 + u, c, p], ibot[16 + u, c, p]], axis=0)
                        down[u, c, p] = jnp.where(top_section, i, v)
                        up[u, c, p] = jnp.where(top_section, v, 0.0)
                    else:
                        top, bot = rest
                        top[u, c, p] = v[0:16]
                        bot[u, c, p] = v[16:32]
        return 0

    lax.fori_loop(0, UNITS // 4, group, 0)


def both_ways(low, high, axis):
    n = lax.axis_size(axis)
    up = [(i, (i + 1) % n) for i in range(n)]
    back = [(t, s) for s, t in up]
    return lax.ppermute(high, axis, up), lax.ppermute(low, axis, back)


def on_device(down_state, up_state, incident, medium_map, media_table, tap_index, kernel_bank):
    SM = pltpu.SMEM
    def half(n):
        return (n, 2, 2, HALF, COLS), f32

    def pack(n):
        return (n // 4, 2, ROWS, COLS), f32

    def full(n):
        return (n, 2, 2, ROWS, COLS), f32

    top, bot = call(halves_body, [half(24)] * 2, [VM] * 3, flops=1 << 20)(
        down_state[0], up_state[0], incident
    )
    first_inc = (top, bot)

    note = jnp.concatenate(
        [medium_map[0], jnp.pad(tap_index, ((0, 7), (0, COLS - 2)))], axis=0
    )
    note = lax.ppermute(note, "depth", [(0, 1), (1, 0)])
    htop, hbot = both_ways(top, bot, "tx")
    amat, bhi, blo, trans, refl = call(
        prep_body,
        [
            ((2, 128, 256), bf16),
            ((2, 384, 256), bf16),
            ((2, 384, 256), bf16),
            ((2, 8, ROWS, COLS), f32),
            ((2, 8, ROWS, COLS), f32),
        ],
        [SM] * 4 + [VM] * 2,
        flops=1 << 28,
    )(
        tap_index,
        note[ROWS : ROWS + 1, 0:2],
        kernel_bank.reshape(-1, TAPS),
        media_table,
        medium_map[0],
        note[0:ROWS],
    )

    def rows(units, odd, *args):
        return call(
            functools.partial(row_body, units // 4, odd),
            [full(units), pack(units), pack(units)],
            [VM] * 5,
            flops=units << 24,
        )(*args)

    w, low, high = rows(24, 0, amat, top, bot, htop, hbot)
    hlow, hhigh = both_ways(low, high, "ty")
    top, bot = call(first_body, [half(UNITS)] * 2, [VM] * 7, flops=1 << 27)(
        bhi, blo, trans, refl, w, hlow, hhigh
    )
    htop, hbot = both_ways(top, bot, "tx")
    const = call(inc_body, [full(UNITS)], [VM] * 6, flops=1 << 26)(bhi, blo, trans, w, hlow, hhigh)[0]
    for tick in range(1, TICKS):
        odd = tick % 2
        last = tick == TICKS - 1
        w, low, high = rows(UNITS, odd, amat, top, bot, htop, hbot)
        hlow, hhigh = both_ways(low, high, "ty")
        args = (bhi, blo, refl, const, w, hlow, hhigh) + (first_inc if last else ())
        outs = [full(UNITS)] * 2 if last else [half(UNITS)] * 2
        res = call(
            functools.partial(next_body, last, odd), outs, [VM] * len(args), flops=1 << 27
        )(*args)
        if not last:
            top, bot = res
            htop, hbot = both_ways(top, bot, "tx")
    return res[0][None], res[1][None]


def solution(mesh):
    in_specs = (
        P("depth", None, None, None, "tx", "ty"),
        P("depth", None, None, None, "tx", "ty"),
        P(None, None, None, "tx", "ty"),
        P("depth", "tx", "ty"),
        P(),
        P("depth", None),
        P(),
    )
    out_specs = (P("depth", None, None, None, "tx", "ty"), P("depth", None, None, None, "tx", "ty"))
    return jax.shard_map(
        on_device, mesh=mesh, in_specs=in_specs, out_specs=out_specs, check_vma=False
    )
```

```python
import functools

import jax
import jax.numpy as jnp
from jax import lax
from jax.experimental import pallas as pl
from jax.experimental.pallas import tpu as pltpu
from jax.sharding import PartitionSpec as P

f32 = jnp.float32
bf16 = jnp.bfloat16
VM = pltpu.VMEM
UNITS = 8
TAPS = 33
HALF = 16
ROWS = 32
COLS = 128


def call(body, outs, ins, flops=0, limit=8, scratch=()):
    return pl.pallas_call(
        body,
        out_shape=[jax.ShapeDtypeStruct(s, d) for s, d in outs],
        in_specs=[pl.BlockSpec(memory_space=m) for m in ins],
        out_specs=[pl.BlockSpec(memory_space=VM)] * len(outs),
        scratch_shapes=list(scratch),
        cost_estimate=pl.CostEstimate(flops=flops, bytes_accessed=0, transcendentals=0),
        compiler_params=pltpu.CompilerParams(vmem_limit_bytes=limit * 1024 * 1024),
    )


def split(x):
    hi = x.astype(bf16)
    lo = (x - hi.astype(f32)).astype(bf16)
    return hi, lo


def dot(a, b):
    return jnp.dot(a, b, preferred_element_type=f32)


def section(odd):
    depth = lax.axis_index("depth")
    return 1 - depth if odd else depth


def band(diff, bank, row):
    re = jnp.zeros(diff.shape, f32)
    im = jnp.zeros(diff.shape, f32)
    for k in range(TAPS):
        hit = diff == k
        re = jnp.where(hit, bank[row, k], re)
        im = jnp.where(hit, bank[row + 1, k], im)
    return re, im


def iota(shape, dim):
    return lax.broadcasted_iota(jnp.int32, shape, dim)


def field(o, n):
    return [[o[(n * 2 + p) * 32 : (n * 2 + p) * 32 + 32, c * 128 : c * 128 + 128] for c in range(2)] for p in range(2)]


def jones(m, v):
    out = []
    for q in range(2):
        re = im = None
        for p in range(2):
            a, b = m[q * 2 + p], m[4 + q * 2 + p]
            r = a * v[p][0] - b * v[p][1]
            i = a * v[p][1] + b * v[p][0]
            re, im = (r, i) if re is None else (re + r, im + i)
        out.append((re, im))
    return out


def halves_body(down, up, top, bot):
    def unit(u, _):
        for n, src in enumerate((down, up)):
            for c in range(2):
                for p in range(2):
                    x = src[u, c, p]
                    top[n * UNITS + u, c, p] = x[0:HALF]
                    bot[n * UNITS + u, c, p] = x[HALF:ROWS]
        return 0

    lax.fori_loop(0, UNITS, unit, 0)


def put(pack, lane16, x, first, k):
    shift = (16 * k - first) % 128
    return jnp.where(lane16 == k, pltpu.roll(x, shift, 1) if shift else x, pack)


def edges_body(inc, mmap, low, high):
    lane16 = iota((ROWS, COLS), 1) >> 4
    zero = jnp.zeros((ROWS, COLS), f32)
    for dst, first in ((low, 0), (high, 112)):
        x = mmap[...].astype(f32)
        pack = zero
        for k in range(8):
            pack = put(pack, lane16, x, first, k)
        dst[4] = pack

    def group(g, _):
        for p in range(2):
            for dst, first in ((low, 0), (high, 112)):
                pack = zero
                for n in range(4):
                    for c in range(2):
                        pack = put(pack, lane16, inc[g * 4 + n, c, p], first, n * 2 + c)
                dst[g * 2 + p] = pack
        return 0

    lax.fori_loop(0, UNITS // 4, group, 0)


def quadrants(re, im, row, col):
    quad = row * 2 + col
    return jnp.where(quad == 1, -im, jnp.where(quad == 2, im, re))


def entries(m, table, first, shape):
    hits = [m == e for e in range(16)]
    out = []
    for q in range(first, first + 8):
        v = jnp.zeros(shape, f32)
        for e in range(16):
            v = jnp.where(hits[e], table[e, q], v)
        if q in (0, 3):
            v = v + 0.5
        out.append(v)
    return out


def prep_body(tap_own, tap_other, bank, table, map_own, map_other, amat, wide, bhi, blo, shi, slo, trans, refl):
    depth = lax.axis_index("depth")
    tx, ty = lax.axis_index("tx"), lax.axis_index("ty")
    tx_low, tx_high = tx == 0, tx == lax.axis_size("tx") - 1
    ty_low, ty_high = ty == 0, ty == lax.axis_size("ty") - 1
    for s in range(2):
        mine = depth == s
        k_row = jnp.where(mine, tap_own[0, 0], tap_other[0, 0]) * 2
        k_col = jnp.where(mine, tap_own[0, 1], tap_other[0, 1]) * 2
        i, j = iota((64, 128), 0), iota((64, 128), 1)
        jj = j & 63
        re, im = band(jj - (i & 31), bank, k_row)
        a = quadrants(re, im, i >> 5, j >> 6)
        gone = ((jj < HALF) & tx_low) | ((jj >= 48) & tx_high)
        a = jnp.where(gone, 0.0, a)
        hi, lo = split(a)
        amat[s, 0:64, 0:128] = hi
        amat[s, 0:64, 128:256] = hi
        amat[s, 64:128, 0:128] = lo
        amat[s, 64:128, 128:256] = jnp.zeros_like(lo)

        for r in range(2):
            i, j = iota((64, 192), 0), iota((64, 192), 1)
            col = (j >= 96).astype(jnp.int32)
            jj = j - 96 * col
            re, im = band(jj - i, bank, k_row)
            a = quadrants(re, im, r, col)
            gone = ((jj < 32) & tx_low) | ((jj >= 64) & tx_high)
            hi, lo = split(jnp.where(gone, 0.0, a))
            wide[s, 0, 64 * r : 64 * r + 64] = hi
            wide[s, 1, 64 * r : 64 * r + 64] = lo

        for part in range(2):
            i, j = iota((64, 128), 1), iota((64, 128), 0) + (HALF + 64 * part)
            re, im = band(j - i, bank, k_col)
            (rh, rl), (ih, il) = split(re), split(im)
            for c, (hr, hm, lr, lm) in enumerate(((rh, ih, rl, il), (-ih, rh, -il, rl))):
                rows = pl.ds(c * 128 + 64 * part, 64)
                bhi[s, rows, 0:128] = hr
                bhi[s, rows, 128:256] = hm
                blo[s, rows, 0:128] = lr
                blo[s, rows, 128:256] = lm
        r, i = iota((64, 128), 0), iota((64, 128), 1)
        side = r >> 5
        re, im = band((r & 15) + side * 144 - i, bank, k_col)
        gone = ((side == 0) & ty_low) | ((side == 1) & ty_high)
        re, im = jnp.where(gone, 0.0, re), jnp.where(gone, 0.0, im)
        isim = ((r >> 4) & 1) == 1
        zero = jnp.zeros((64, 128), bf16)
        for n, v in enumerate((jnp.where(isim, -im, re), jnp.where(isim, re, im))):
            hi, lo = split(v)
            cols = pl.ds(n * 128, 128)
            bhi[s, 256:320, cols] = hi
            blo[s, 256:320, cols] = lo
            bhi[s, 320:384, cols] = zero
            blo[s, 320:384, cols] = zero

        m = jnp.where(mine, map_own[...], map_other[...])
        for q, v in enumerate(entries(m, table, 0, (ROWS, COLS))):
            trans[s, q] = v
        for q, v in enumerate(entries(m, table, 8, (ROWS, COLS))):
            refl[s, q] = v if s == 0 else -v

    for part in range(6):
        r, j = iota((64, 128), 0) + 64 * part, iota((64, 128), 1)
        l = (r >> 7) * 16 + (r & 15)
        diff = jnp.where(((r >> 5) & 3) == (j >> 5), l - (j & 15), -1)
        re, im = band(diff, bank, tap_own[0, 1] * 2)
        a = quadrants(re, im, (j >> 4) & 1, (r >> 4) & 1)
        hi, lo = split(a)
        shi[64 * part : 64 * part + 64] = hi
        slo[64 * part : 64 * part + 64] = lo


def strips_body(table, elow, ehigh, trans, refl):
    sign = jnp.where(section(0) == 0, 1.0, -1.0).astype(f32)
    im = ((iota((ROWS, COLS), 1) >> 4) & 1) == 1
    for side, e in enumerate((elow, ehigh)):
        m = (e[4] + 0.5).astype(jnp.int32)
        for dst, first, factor in ((trans, 0, 1.0), (refl, 8, sign)):
            for q, v in enumerate(entries(m, table, first, (ROWS, COLS))):
                v = v * factor
                dst[side, q] = v if q < 4 else jnp.where(im, v, -v)


def taller_body(table, trans, refl, utop, ubot, tall_t, tall_r):
    o = section(1)
    sign = jnp.where(o == 0, 1.0, -1.0).astype(f32)
    for q in range(8):
        tall_t[q, 16:48] = trans[0, q]
        tall_r[q, 16:48] = refl[o, q]
    for dst, x in ((0, utop[32, 16:32]), (48, ubot[32, 0:16])):
        m = (x + 0.5).astype(jnp.int32)
        for q, v in enumerate(entries(m, table, 0, (16, COLS))):
            tall_t[q, dst : dst + 16] = v
        for q, v in enumerate(entries(m, table, 8, (16, COLS))):
            tall_r[q, dst : dst + 16] = v * sign


def stack(rows):
    return jnp.concatenate(
        [jnp.concatenate([r(c, p) for p in range(2)], axis=1) for c in range(2) for r in rows], axis=0
    )


def narrow(lhs, v):
    hi, lo = split(v)
    o = dot(lhs, jnp.concatenate([hi, lo], axis=0))
    return o[0:64] + o[64:128]


def broad(hi, lo, v):
    vh, vl = split(v)
    return dot(hi, vh) + dot(hi, vl) + dot(lo, vh)


def part(o, rows, c, p):
    return o[c * rows : c * rows + rows, p * 128 : p * 128 + 128]


def fields(o, rows):
    return [[part(o, rows, c, p) for c in range(2)] for p in range(2)]


EDGES = ((0, 16), (112, 96))


def row_body(amat, top, bot, htop, hbot, w, low, high):
    lane16 = iota((ROWS, COLS), 1) >> 4
    lhs = amat[section(0)]

    def group(g, _):
        packs = [[[jnp.zeros((ROWS, COLS), f32) for _ in range(2)] for _ in range(2)] for _ in range(2)]
        for n in range(4):
            u = g * 4 + n
            o = narrow(lhs, stack([lambda c, p, x=x: x[u, c, p] for x in (htop, top, bot, hbot)]))
            for c in range(2):
                for p in range(2):
                    x = part(o, 32, c, p)
                    w[u, c, p] = x
                    for side in range(2):
                        for far in range(2):
                            packs[side][far][p] = put(packs[side][far][p], lane16, x, EDGES[side][far], n * 2 + c)
        for p in range(2):
            for far in range(2):
                low[far, g, p] = packs[0][far][p]
                high[far, g, p] = packs[1][far][p]
        return 0

    lax.fori_loop(0, 2 * UNITS // 4, group, 0)


def columns(w, hlow, hhigh, g, bh, bl):
    lane = iota((ROWS, COLS), 1)
    rows = []
    for n in range(4):
        for p in range(2):
            a, b = hlow(g, p), hhigh(g, p)
            a = pltpu.roll(a, 128 - 32 * n, 1) if n else a
            b = pltpu.roll(b, (160 - 32 * n) % 128, 1) if n != 1 else b
            u = g * 4 + n
            rows.append(jnp.concatenate([w[u, 0, p], w[u, 1, p], jnp.where(lane < 32, a, b)], axis=1))
    hi, lo = split(jnp.concatenate(rows, axis=0))
    return dot(hi, bh) + dot(lo, bh) + dot(hi, bl)


def inc_column_body(bhi, blo, inc, elow, ehigh, map_other, out):
    bh, bl = bhi[0], blo[0]

    def group(g, _):
        o = columns(inc, lambda g, p: elow[g * 2 + p], lambda g, p: ehigh[g * 2 + p], g, bh, bl)
        for n in range(4):
            f = field(o, n)
            for c in range(2):
                for p in range(2):
                    out[(g * 4 + n) * 4 + c * 2 + p] = f[p][c]
        return 0

    lax.fori_loop(0, UNITS // 4, group, 0)
    out[32] = map_other[...].astype(f32)


def inc_row_body(wide, tall_t, x, utop, ubot, const):
    hi, lo = wide[0, 0], wide[0, 1]

    def unit(u, _):
        o = broad(hi, lo, stack([lambda c, p, y=y: y[u * 4 + c * 2 + p] for y in (utop, x, ubot)]))
        a = jones([tall_t[q] for q in range(8)], fields(o, 64))
        for p in range(2):
            for c in range(2):
                const[u, c, p] = a[p][c]
        return 0

    lax.fori_loop(0, UNITS, unit, 0)


def column_body(first, bhi, blo, shi, slo, trans, refl, strans, srefl, const, w, low, high, hlow, hhigh, *rest):
    out, mid, slow, shigh = rest[-4:]
    outs = rest[:-4] + (out,)
    d = section(0)
    gate = jnp.where(d == 0, 1.0, 0.0).astype(f32)
    sh, sl = shi[...], slo[...]
    im = ((iota((ROWS, COLS), 1) >> 4) & 1) == 1

    def swapped(x):
        return jnp.where(im, pltpu.roll(x, 16, 1), pltpu.roll(x, 112, 1))

    def group_of(which, g):
        if not first:
            return g
        return (d if which == 0 else 1 - d) * 2 + g

    def strip_group(g, _):
        rows = []
        for side in range(2):
            for which in range(2 if first else 1):
                k = group_of(which, g)
                for p in range(2):
                    if side == 0:
                        x = (hlow[1, k, p], hlow[0, k, p], low[0, k, p])
                    else:
                        x = (high[0, k, p], hhigh[0, k, p], hhigh[1, k, p])
                    rows.append(jnp.concatenate(x, axis=1))
        hi, lo = split(jnp.concatenate(rows, axis=0))
        o = dot(hi, sh) + dot(lo, sh) + dot(hi, sl)
        n = 0
        for side in range(2):
            mats = (strans, srefl) if first else (srefl,)
            acc = [jnp.zeros((ROWS, COLS), f32)] * 2
            for m in mats:
                for p in range(2):
                    x = o[n * 32 : n * 32 + 32]
                    n += 1
                    y = swapped(x)
                    for q in range(2):
                        acc[q] = acc[q] + m[side, q * 2 + p] * x + m[side, 4 + q * 2 + p] * y
            for q in range(2):
                dst, halo = ((slow, hlow), (shigh, hhigh))[side]
                dst[g, q] = acc[q] if first else acc[q] + gate * halo[2, g, q]
        return 0

    lax.fori_loop(0, UNITS // 4, strip_group, 0)
    bh, bl = bhi[d], blo[d]

    def main_group(g, _):
        os = [
            columns(w, lambda g, p: hlow[0, g, p], lambda g, p: hhigh[0, g, p], group_of(k, g), bh, bl)
            for k in range(2 if first else 1)
        ]
        for n in range(4):
            u = g * 4 + n
            b = jones([refl[d, q] for q in range(8)], field(os[-1], n))
            if first:
                a = jones([trans[d, q] for q in range(8)], field(os[0], n))
            for p in range(2):
                for c in range(2):
                    extra = a[p][c] if first else gate * const[u, c, p, 16:48]
                    mid[u, c, p] = b[p][c] + extra
        return 0

    lax.fori_loop(0, UNITS // 4, main_group, 0)
    ch, cl = bhi[1 - d], blo[1 - d]

    def next_group(g, _):
        o = columns(mid, lambda g, p: slow[g, p], lambda g, p: shigh[g, p], g, ch, cl)
        for n in range(4):
            f = field(o, n)
            for c in range(2):
                for p in range(2):
                    if first:
                        out[g * 4 + n, c, p] = f[p][c]
                    else:
                        outs[0][g * 4 + n, c, p] = f[p][c][0:16]
                        outs[1][g * 4 + n, c, p] = f[p][c][16:32]
        return 0

    lax.fori_loop(0, UNITS // 4, next_group, 0)


def second_body(amat, wide, tall_r, const, x, htop, hbot, w, low, high):
    lane16 = iota((ROWS, COLS), 1) >> 4
    d, o = section(0), section(1)
    gate = jnp.where(o == 0, 1.0, 0.0).astype(f32)
    lhs = amat[d]
    hi, lo = wide[o, 0], wide[o, 1]

    def group(g, _):
        packs = [[[jnp.zeros((ROWS, COLS), f32) for _ in range(2)] for _ in range(3)] for _ in range(2)]
        for n in range(4):
            u = g * 4 + n
            v = broad(hi, lo, stack([lambda c, p, y=y: y[u, c, p] for y in (htop, x, hbot)]))
            b = jones([tall_r[q] for q in range(8)], fields(v, 64))
            v = narrow(lhs, stack([lambda c, p: b[p][c] + gate * const[u, c, p]]))
            for c in range(2):
                for p in range(2):
                    y = part(v, 32, c, p)
                    w[u, c, p] = y
                    z = const[u, c, p, 16:48]
                    for side in range(2):
                        for far in range(3):
                            packs[side][far][p] = put(
                                packs[side][far][p],
                                lane16,
                                z if far == 2 else y,
                                EDGES[side][far % 2],
                                n * 2 + c,
                            )
        for p in range(2):
            for far in range(3):
                low[far, g, p] = packs[0][far][p]
                high[far, g, p] = packs[1][far][p]
        return 0

    lax.fori_loop(0, UNITS // 4, group, 0)


def last_body(amat, refl, const, inc, top, bot, htop, hbot, down, up):
    o = section(1)
    gate = jnp.where(o == 0, 1.0, 0.0).astype(f32)
    top_section = lax.axis_index("depth") == 0
    lhs = amat[o]

    def unit(u, _):
        v = narrow(lhs, stack([lambda c, p, x=x: x[u, c, p] for x in (htop, top, bot, hbot)]))
        b = jones([refl[o, q] for q in range(8)], fields(v, 32))
        for p in range(2):
            for c in range(2):
                y = b[p][c] + gate * const[u, c, p, 16:48]
                down[u, c, p] = jnp.where(top_section, inc[u, c, p], y)
                up[u, c, p] = jnp.where(top_section, y, 0.0)
        return 0

    lax.fori_loop(0, UNITS, unit, 0)


def both_ways(low, high, axis):
    n = lax.axis_size(axis)
    up = [(i, (i + 1) % n) for i in range(n)]
    back = [(t, s) for s, t in up]
    return lax.ppermute(high, axis, up), lax.ppermute(low, axis, back)


def on_device(down_state, up_state, incident, medium_map, media_table, tap_index, kernel_bank):
    SM = pltpu.SMEM

    def half(n):
        return (n, 2, 2, HALF, COLS), f32

    def full(n):
        return (n, 2, 2, ROWS, COLS), f32

    def packs(kinds, n):
        return (kinds, n // 4, 2, ROWS, COLS), f32

    def planes(*n):
        return n + (ROWS, COLS), f32

    top, bot = call(halves_body, [half(16)] * 2, [VM] * 2, flops=1 << 20)(down_state[0], up_state[0])
    htop, hbot = both_ways(top, bot, "tx")

    note = jnp.concatenate([medium_map[0], jnp.pad(tap_index, ((0, 7), (0, COLS - 2)))], axis=0)
    note = lax.ppermute(note, "depth", [(0, 1), (1, 0)])
    map_other = note[0:ROWS]
    elow, ehigh = both_ways(
        *call(edges_body, [planes(5)] * 2, [VM] * 2, flops=1 << 20)(incident, medium_map[0]), "ty"
    )
    amat, wide, bhi, blo, shi, slo, trans, refl = call(
        prep_body,
        [
            ((2, 128, 256), bf16),
            ((2, 2, 128, 192), bf16),
            ((2, 384, 256), bf16),
            ((2, 384, 256), bf16),
            ((384, 128), bf16),
            ((384, 128), bf16),
            planes(2, 8),
            planes(2, 8),
        ],
        [SM] * 4 + [VM] * 2,
        flops=1 << 27,
    )(
        tap_index,
        note[ROWS : ROWS + 1, 0:2],
        kernel_bank.reshape(-1, TAPS),
        media_table,
        medium_map[0],
        map_other,
    )
    strans, srefl = call(strips_body, [planes(2, 8)] * 2, [SM] + [VM] * 2, flops=1 << 25)(
        media_table, elow, ehigh
    )
    inc_cols = call(inc_column_body, [planes(33)], [VM] * 6, flops=1 << 26)(
        bhi, blo, incident, elow, ehigh, map_other
    )[0]

    htop, hbot, inc_cols = lax.optimization_barrier((htop, hbot, inc_cols))
    w, low, high = call(row_body, [full(16)] + [packs(2, 16)] * 2, [VM] * 5, flops=1 << 27)(
        amat, top, bot, htop, hbot
    )
    low, high, inc_cols = lax.optimization_barrier((low, high, inc_cols))
    hlow, hhigh = both_ways(low, high, "ty")
    utop, ubot = both_ways(inc_cols, inc_cols, "tx")

    def two_ticks(first, outs, *args):
        scratch = [VM(*full(UNITS)), VM((2, 2, ROWS, COLS), f32), VM((2, 2, ROWS, COLS), f32)]
        return call(functools.partial(column_body, first), outs, [VM] * len(args), flops=1 << 27, scratch=scratch)(*args)

    mats = (bhi, blo, shi, slo, trans, refl, strans, srefl)
    x = two_ticks(True, [full(UNITS)], *mats, trans, w, low, high, hlow, hhigh)[0]
    htop, hbot = both_ways(x, x, "tx")
    tall = ((8, 64, COLS), f32)
    tall_t, tall_r = call(taller_body, [tall] * 2, [SM] + [VM] * 4, flops=1 << 25)(
        media_table, trans, refl, utop, ubot
    )
    const = call(inc_row_body, [((UNITS, 2, 2, 64, COLS), f32)], [VM] * 5, flops=1 << 26)(
        wide, tall_t, inc_cols, utop, ubot
    )[0]
    w, low, high = call(second_body, [full(UNITS)] + [packs(3, UNITS)] * 2, [VM] * 7, flops=1 << 27)(
        amat, wide, tall_r, const, x, htop, hbot
    )
    hlow, hhigh = both_ways(low, high, "ty")
    top, bot = two_ticks(False, [half(UNITS)] * 2, *mats, const, w, low, high, hlow, hhigh)
    htop, hbot = both_ways(top, bot, "tx")
    down, up = call(last_body, [full(UNITS)] * 2, [VM] * 8, flops=1 << 27)(
        amat, refl, const, incident, top, bot, htop, hbot
    )
    return down[None], up[None]


def solution(mesh):
    in_specs = (
        P("depth", None, None, None, "tx", "ty"),
        P("depth", None, None, None, "tx", "ty"),
        P(None, None, None, "tx", "ty"),
        P("depth", "tx", "ty"),
        P(),
        P("depth", None),
        P(),
    )
    out_specs = (P("depth", None, None, None, "tx", "ty"), P("depth", None, None, None, "tx", "ty"))
    return jax.shard_map(
        on_device, mesh=mesh, in_specs=in_specs, out_specs=out_specs, check_vma=False
    )
```

```python
import functools

import jax
import jax.numpy as jnp
from jax import lax
from jax.experimental import pallas as pl
from jax.experimental.pallas import tpu as pltpu
from jax.sharding import PartitionSpec as P

f32 = jnp.float32
bf16 = jnp.bfloat16
VM = pltpu.VMEM
UNITS = 8
TAPS = 33
HALF = 16
ROWS = 32
COLS = 128


def call(body, outs, ins, flops=0, limit=8, scratch=(), home=VM):
    return pl.pallas_call(
        body,
        out_shape=[jax.ShapeDtypeStruct(s, d) for s, d in outs],
        in_specs=[pl.BlockSpec(memory_space=m) for m in ins],
        out_specs=[pl.BlockSpec(memory_space=home)] * len(outs),
        scratch_shapes=list(scratch),
        cost_estimate=pl.CostEstimate(flops=flops, bytes_accessed=0, transcendentals=0),
        compiler_params=pltpu.CompilerParams(vmem_limit_bytes=limit * 1024 * 1024),
    )


def split(x):
    hi = x.astype(bf16)
    lo = (x - hi.astype(f32)).astype(bf16)
    return hi, lo


def dot(a, b):
    return jnp.dot(a, b, preferred_element_type=f32)


def section(odd):
    depth = lax.axis_index("depth")
    return 1 - depth if odd else depth


def band(diff, bank, row):
    re = jnp.zeros(diff.shape, f32)
    im = jnp.zeros(diff.shape, f32)
    for k in range(TAPS):
        hit = diff == k
        re = jnp.where(hit, bank[row, k], re)
        im = jnp.where(hit, bank[row + 1, k], im)
    return re, im


def iota(shape, dim):
    return lax.broadcasted_iota(jnp.int32, shape, dim)


def field(o, n):
    return [[o[(n * 2 + p) * 32 : (n * 2 + p) * 32 + 32, c * 128 : c * 128 + 128] for c in range(2)] for p in range(2)]


def jones(m, v):
    out = []
    for q in range(2):
        re = im = None
        for p in range(2):
            a, b = m[q * 2 + p], m[4 + q * 2 + p]
            r = a * v[p][0] - b * v[p][1]
            i = a * v[p][1] + b * v[p][0]
            re, im = (r, i) if re is None else (re + r, im + i)
        out.append((re, im))
    return out


def halves_body(down, up, top, bot):
    def unit(u, _):
        for n, src in enumerate((down, up)):
            for c in range(2):
                for p in range(2):
                    x = src[u, c, p]
                    top[n * UNITS + u, c, p] = x[0:HALF]
                    bot[n * UNITS + u, c, p] = x[HALF:ROWS]
        return 0

    lax.fori_loop(0, UNITS, unit, 0)


def put(pack, lane16, x, first, k):
    shift = (16 * k - first) % 128
    return jnp.where(lane16 == k, pltpu.roll(x, shift, 1) if shift else x, pack)


def edges_body(inc, mmap, low, high):
    lane16 = iota((ROWS, COLS), 1) >> 4
    zero = jnp.zeros((ROWS, COLS), f32)
    for dst, first in ((low, 0), (high, 112)):
        x = mmap[...].astype(f32)
        pack = zero
        for k in range(8):
            pack = put(pack, lane16, x, first, k)
        dst[4] = pack

    def group(g, _):
        for p in range(2):
            for dst, first in ((low, 0), (high, 112)):
                pack = zero
                for n in range(4):
                    for c in range(2):
                        pack = put(pack, lane16, inc[g * 4 + n, c, p], first, n * 2 + c)
                dst[g * 2 + p] = pack
        return 0

    lax.fori_loop(0, UNITS // 4, group, 0)


def quadrants(re, im, row, col):
    quad = row * 2 + col
    return jnp.where(quad == 1, -im, jnp.where(quad == 2, im, re))


def entries(m, table, first, shape):
    hits = [m == e for e in range(16)]
    out = []
    for q in range(first, first + 8):
        v = jnp.zeros(shape, f32)
        for e in range(16):
            v = jnp.where(hits[e], table[e, q], v)
        if q in (0, 3):
            v = v + 0.5
        out.append(v)
    return out


def tables(slot, tap, bank, table, m, sign, amat, bhi, blo, trans, refl):
    tx, ty = lax.axis_index("tx"), lax.axis_index("ty")
    tx_low, tx_high = tx == 0, tx == lax.axis_size("tx") - 1
    ty_low, ty_high = ty == 0, ty == lax.axis_size("ty") - 1
    k_row, k_col = tap[0, 0] * 2, tap[0, 1] * 2
    i, j = iota((64, 128), 0), iota((64, 128), 1)
    jj = j & 63
    re, im = band(jj - (i & 31), bank, k_row)
    a = quadrants(re, im, i >> 5, j >> 6)
    gone = ((jj < HALF) & tx_low) | ((jj >= 48) & tx_high)
    a = jnp.where(gone, 0.0, a)
    hi, lo = split(a)
    amat[slot, 0:64, 0:128] = hi
    amat[slot, 0:64, 128:256] = hi
    amat[slot, 64:128, 0:128] = lo
    amat[slot, 64:128, 128:256] = jnp.zeros_like(lo)

    for part in range(2):
        i, j = iota((64, 128), 1), iota((64, 128), 0) + (HALF + 64 * part)
        re, im = band(j - i, bank, k_col)
        (rh, rl), (ih, il) = split(re), split(im)
        for c, (hr, hm, lr, lm) in enumerate(((rh, ih, rl, il), (-ih, rh, -il, rl))):
            rows = pl.ds(c * 128 + 64 * part, 64)
            bhi[slot, rows, 0:128] = hr
            bhi[slot, rows, 128:256] = hm
            blo[slot, rows, 0:128] = lr
            blo[slot, rows, 128:256] = lm
    r, i = iota((64, 128), 0), iota((64, 128), 1)
    side = r >> 5
    re, im = band((r & 15) + side * 144 - i, bank, k_col)
    gone = ((side == 0) & ty_low) | ((side == 1) & ty_high)
    re, im = jnp.where(gone, 0.0, re), jnp.where(gone, 0.0, im)
    isim = ((r >> 4) & 1) == 1
    zero = jnp.zeros((64, 128), bf16)
    for n, v in enumerate((jnp.where(isim, -im, re), jnp.where(isim, re, im))):
        hi, lo = split(v)
        cols = pl.ds(n * 128, 128)
        bhi[slot, 256:320, cols] = hi
        blo[slot, 256:320, cols] = lo
        bhi[slot, 320:384, cols] = zero
        blo[slot, 320:384, cols] = zero

    for q, v in enumerate(entries(m, table, 0, (ROWS, COLS))):
        trans[slot, q] = v
    for q, v in enumerate(entries(m, table, 8, (ROWS, COLS))):
        refl[slot, q] = v * sign


def sign_of(sec):
    return jnp.where(sec == 0, 1.0, -1.0).astype(f32)


def own_body(tap, bank, table, mmap, amat, bhi, blo, trans, refl, shi, slo):
    tables(0, tap, bank, table, mmap[...], sign_of(section(0)), amat, bhi, blo, trans, refl)
    for part in range(6):
        r, j = iota((64, 128), 0) + 64 * part, iota((64, 128), 1)
        l = (r >> 7) * 16 + (r & 15)
        diff = jnp.where(((r >> 5) & 3) == (j >> 5), l - (j & 15), -1)
        re, im = band(diff, bank, tap[0, 1] * 2)
        a = quadrants(re, im, (j >> 4) & 1, (r >> 4) & 1)
        hi, lo = split(a)
        shi[64 * part : 64 * part + 64] = hi
        slo[64 * part : 64 * part + 64] = lo


def other_body(tap, bank, table, mmap, *refs):
    own, both = refs[:5], refs[5:]
    o = section(1)
    for x, y in zip(own, both):
        y[1 - o] = x[0]
    tables(o, tap, bank, table, mmap[...], sign_of(o), *both)


def wide_body(tap_own, tap_other, bank, x, wide):
    depth, tx = lax.axis_index("depth"), lax.axis_index("tx")
    tx_low, tx_high = tx == 0, tx == lax.axis_size("tx") - 1
    for s in range(2):
        k_row = jnp.where(depth == s, tap_own[0, 0], tap_other[0, 0]) * 2
        i, j = iota((64, 96), 0), iota((64, 96), 1)
        re, im = band(j - i, bank, k_row)
        gone = ((j < 32) & tx_low) | ((j >= 64) & tx_high)
        re, im = jnp.where(gone, 0.0, re), jnp.where(gone, 0.0, im)
        for r in range(2):
            row = (re, -im) if r == 0 else (im, re)
            hi, lo = split(jnp.concatenate(row, axis=1))
            wide[s, 0, 64 * r : 64 * r + 64] = hi
            wide[s, 1, 64 * r : 64 * r + 64] = lo


def strips_body(table, elow, ehigh, trans, refl):
    sign = sign_of(section(0))
    im = ((iota((ROWS, COLS), 1) >> 4) & 1) == 1
    for side, e in enumerate((elow, ehigh)):
        m = (e[4] + 0.5).astype(jnp.int32)
        for dst, first, factor in ((trans, 0, 1.0), (refl, 8, sign)):
            for q, v in enumerate(entries(m, table, first, (ROWS, COLS))):
                v = v * factor
                dst[side, q] = v if q < 4 else jnp.where(im, v, -v)


def taller_body(table, trans, refl, utop, ubot, tall_t, tall_r):
    o = section(1)
    sign = sign_of(o)
    for q in range(8):
        tall_t[q, 16:48] = trans[0, q]
        tall_r[q, 16:48] = refl[o, q]
    for dst, x in ((0, utop[32, 16:32]), (48, ubot[32, 0:16])):
        m = (x + 0.5).astype(jnp.int32)
        for q, v in enumerate(entries(m, table, 0, (16, COLS))):
            tall_t[q, dst : dst + 16] = v
        for q, v in enumerate(entries(m, table, 8, (16, COLS))):
            tall_r[q, dst : dst + 16] = v * sign


def stack(rows):
    return jnp.concatenate(
        [jnp.concatenate([r(c, p) for p in range(2)], axis=1) for c in range(2) for r in rows], axis=0
    )


def narrow(lhs, v):
    hi, lo = split(v)
    o = dot(lhs, jnp.concatenate([hi, lo], axis=0))
    return o[0:64] + o[64:128]


def broad(hi, lo, v):
    vh, vl = split(v)
    return dot(hi, vh) + dot(hi, vl) + dot(lo, vh)


def part(o, rows, c, p):
    return o[c * rows : c * rows + rows, p * 128 : p * 128 + 128]


def fields(o, rows):
    return [[part(o, rows, c, p) for c in range(2)] for p in range(2)]


EDGES = ((0, 16), (112, 96))


def row_body(amat, top, bot, htop, hbot, w, low, high):
    lane16 = iota((ROWS, COLS), 1) >> 4
    lhs = amat[0]

    def group(g, _):
        packs = [[[jnp.zeros((ROWS, COLS), f32) for _ in range(2)] for _ in range(2)] for _ in range(2)]
        for n in range(4):
            u = g * 4 + n
            o = narrow(lhs, stack([lambda c, p, x=x: x[u, c, p] for x in (htop, top, bot, hbot)]))
            for c in range(2):
                for p in range(2):
                    x = part(o, 32, c, p)
                    w[u, c, p] = x
                    for side in range(2):
                        for far in range(2):
                            packs[side][far][p] = put(packs[side][far][p], lane16, x, EDGES[side][far], n * 2 + c)
        for p in range(2):
            for far in range(2):
                low[far, g, p] = packs[0][far][p]
                high[far, g, p] = packs[1][far][p]
        return 0

    lax.fori_loop(0, 2 * UNITS // 4, group, 0)


def columns(w, hlow, hhigh, g, bh, bl):
    lane = iota((ROWS, COLS), 1)
    rows = []
    for n in range(4):
        for p in range(2):
            a, b = hlow(g, p), hhigh(g, p)
            a = pltpu.roll(a, 128 - 32 * n, 1) if n else a
            b = pltpu.roll(b, (160 - 32 * n) % 128, 1) if n != 1 else b
            u = g * 4 + n
            rows.append(jnp.concatenate([w[u, 0, p], w[u, 1, p], jnp.where(lane < 32, a, b)], axis=1))
    hi, lo = split(jnp.concatenate(rows, axis=0))
    return dot(hi, bh) + dot(lo, bh) + dot(hi, bl)


def inc_column_body(bhi, blo, inc, elow, ehigh, map_other, out):
    bh, bl = bhi[0], blo[0]

    def group(g, _):
        o = columns(inc, lambda g, p: elow[g * 2 + p], lambda g, p: ehigh[g * 2 + p], g, bh, bl)
        for n in range(4):
            f = field(o, n)
            for c in range(2):
                for p in range(2):
                    out[(g * 4 + n) * 4 + c * 2 + p] = f[p][c]
        return 0

    lax.fori_loop(0, UNITS // 4, group, 0)
    out[32] = map_other[...].astype(f32)


def inc_row_body(wide, tall_t, x, utop, ubot, const):
    hi, lo = wide[0, 0], wide[0, 1]

    def group(g, _):
        for u in [g * 4 + n for n in range(4)]:
            o = broad(hi, lo, stack([lambda c, p, y=y: y[u * 4 + c * 2 + p] for y in (utop, x, ubot)]))
            a = jones([tall_t[q] for q in range(8)], fields(o, 64))
            for p in range(2):
                for c in range(2):
                    const[u, c, p] = a[p][c]
        return 0

    lax.fori_loop(0, UNITS // 4, group, 0)


def column_body(first, bhi, blo, shi, slo, trans, refl, strans, srefl, const, w, low, high, hlow, hhigh, *rest):
    out, mid, slow, shigh = rest[-4:]
    outs = rest[:-4] + (out,)
    d = section(0)
    gate = jnp.where(d == 0, 1.0, 0.0).astype(f32)
    sh, sl = shi[...], slo[...]
    im = ((iota((ROWS, COLS), 1) >> 4) & 1) == 1

    def swapped(x):
        return jnp.where(im, pltpu.roll(x, 16, 1), pltpu.roll(x, 112, 1))

    def group_of(which, g):
        if not first:
            return g
        return (d if which == 0 else 1 - d) * 2 + g

    def strip_group(g, _):
        rows = []
        for side in range(2):
            for which in range(2 if first else 1):
                k = group_of(which, g)
                for p in range(2):
                    if side == 0:
                        x = (hlow[1, k, p], hlow[0, k, p], low[0, k, p])
                    else:
                        x = (high[0, k, p], hhigh[0, k, p], hhigh[1, k, p])
                    rows.append(jnp.concatenate(x, axis=1))
        hi, lo = split(jnp.concatenate(rows, axis=0))
        o = dot(hi, sh) + dot(lo, sh) + dot(hi, sl)
        n = 0
        for side in range(2):
            mats = (strans, srefl) if first else (srefl,)
            acc = [jnp.zeros((ROWS, COLS), f32)] * 2
            for m in mats:
                for p in range(2):
                    x = o[n * 32 : n * 32 + 32]
                    n += 1
                    y = swapped(x)
                    for q in range(2):
                        acc[q] = acc[q] + m[side, q * 2 + p] * x + m[side, 4 + q * 2 + p] * y
            for q in range(2):
                dst, halo = ((slow, hlow), (shigh, hhigh))[side]
                dst[g, q] = acc[q] if first else acc[q] + gate * halo[2, g, q]
        return 0

    lax.fori_loop(0, UNITS // 4, strip_group, 0)
    bh, bl = bhi[d], blo[d]

    def main_group(g, _):
        os = [
            columns(w, lambda g, p: hlow[0, g, p], lambda g, p: hhigh[0, g, p], group_of(k, g), bh, bl)
            for k in range(2 if first else 1)
        ]
        for n in range(4):
            u = g * 4 + n
            b = jones([refl[d, q] for q in range(8)], field(os[-1], n))
            if first:
                a = jones([trans[d, q] for q in range(8)], field(os[0], n))
            for p in range(2):
                for c in range(2):
                    extra = a[p][c] if first else gate * const[u, c, p, 16:48]
                    mid[u, c, p] = b[p][c] + extra
        return 0

    lax.fori_loop(0, UNITS // 4, main_group, 0)
    ch, cl = bhi[1 - d], blo[1 - d]

    def next_group(g, _):
        o = columns(mid, lambda g, p: slow[g, p], lambda g, p: shigh[g, p], g, ch, cl)
        for n in range(4):
            f = field(o, n)
            for c in range(2):
                for p in range(2):
                    if first:
                        out[g * 4 + n, c, p] = f[p][c]
                    else:
                        outs[0][g * 4 + n, c, p] = f[p][c][0:16]
                        outs[1][g * 4 + n, c, p] = f[p][c][16:32]
        return 0

    lax.fori_loop(0, UNITS // 4, next_group, 0)


def second_body(amat, wide, tall_r, const, x, htop, hbot, w, low, high):
    lane16 = iota((ROWS, COLS), 1) >> 4
    d, o = section(0), section(1)
    gate = jnp.where(o == 0, 1.0, 0.0).astype(f32)
    lhs = amat[d]
    hi, lo = wide[o, 0], wide[o, 1]

    def group(g, _):
        packs = [[[jnp.zeros((ROWS, COLS), f32) for _ in range(2)] for _ in range(3)] for _ in range(2)]
        for n in range(4):
            u = g * 4 + n
            v = broad(hi, lo, stack([lambda c, p, y=y: y[u, c, p] for y in (htop, x, hbot)]))
            b = jones([tall_r[q] for q in range(8)], fields(v, 64))
            v = narrow(lhs, stack([lambda c, p: b[p][c] + gate * const[u, c, p]]))
            for c in range(2):
                for p in range(2):
                    y = part(v, 32, c, p)
                    w[u, c, p] = y
                    z = const[u, c, p, 16:48]
                    for side in range(2):
                        for far in range(3):
                            packs[side][far][p] = put(
                                packs[side][far][p],
                                lane16,
                                z if far == 2 else y,
                                EDGES[side][far % 2],
                                n * 2 + c,
                            )
        for p in range(2):
            for far in range(3):
                low[far, g, p] = packs[0][far][p]
                high[far, g, p] = packs[1][far][p]
        return 0

    lax.fori_loop(0, UNITS // 4, group, 0)


def last_body(amat, refl, const, inc, top, bot, htop, hbot, down, up, vdown, vup, sems):
    o = section(1)
    gate = jnp.where(o == 0, 1.0, 0.0).astype(f32)
    top_section = lax.axis_index("depth") == 0
    lhs = amat[o]
    copies = []
    for g in range(UNITS // 2):
        for u in (g * 2, g * 2 + 1):
            v = narrow(lhs, stack([lambda c, p, x=x: x[u, c, p] for x in (htop, top, bot, hbot)]))
            b = jones([refl[o, q] for q in range(8)], fields(v, 32))
            for p in range(2):
                for c in range(2):
                    y = b[p][c] + gate * const[u, c, p, 16:48]
                    vdown[u, c, p] = jnp.where(top_section, inc[u, c, p], y)
                    vup[u, c, p] = jnp.where(top_section, y, 0.0)
        for n, (src, dst) in enumerate(((vdown, down), (vup, up))):
            copy = pltpu.make_async_copy(src.at[pl.ds(g * 2, 2)], dst.at[pl.ds(g * 2, 2)], sems.at[2 * g + n])
            copy.start()
            copies.append(copy)
    for copy in copies:
        copy.wait()


def both_ways(low, high, axis):
    n = lax.axis_size(axis)
    up = [(i, (i + 1) % n) for i in range(n)]
    back = [(t, s) for s, t in up]
    return lax.ppermute(high, axis, up), lax.ppermute(low, axis, back)


def on_device(down_state, up_state, incident, medium_map, media_table, tap_index, kernel_bank):
    SM = pltpu.SMEM

    def half(n):
        return (n, 2, 2, HALF, COLS), f32

    def full(n):
        return (n, 2, 2, ROWS, COLS), f32

    def packs(kinds, n):
        return (kinds, n // 4, 2, ROWS, COLS), f32

    def planes(*n):
        return n + (ROWS, COLS), f32

    top, bot = call(halves_body, [half(16)] * 2, [VM] * 2, flops=1 << 20)(down_state[0], up_state[0])
    bank = kernel_bank.reshape(-1, TAPS)
    htop, hbot = both_ways(top, bot, "tx")
    elow, ehigh = both_ways(
        *call(edges_body, [planes(5)] * 2, [VM] * 2, flops=1 << 20)(incident, medium_map[0]), "ty"
    )
    note = jnp.concatenate([medium_map[0], jnp.pad(tap_index, ((0, 7), (0, COLS - 2)))], axis=0)
    note = lax.ppermute(note, "depth", [(0, 1), (1, 0)])

    def lookups(n):
        return [((n, 128, 256), bf16)] + [((n, 384, 256), bf16)] * 2 + [planes(n, 8)] * 2

    *own, shi, slo = call(own_body, lookups(1) + [((384, 128), bf16)] * 2, [SM] * 3 + [VM], flops=1 << 27)(
        tap_index, bank, media_table, medium_map[0]
    )
    htop, hbot, elow, ehigh, note = lax.optimization_barrier((htop, hbot, elow, ehigh, note))
    w, low, high = call(row_body, [full(16)] + [packs(2, 16)] * 2, [VM] * 5, flops=1 << 27)(
        own[0], top, bot, htop, hbot
    )
    low, high, note, elow, ehigh = lax.optimization_barrier((low, high, note, elow, ehigh))
    hlow, hhigh = both_ways(low, high, "ty")
    map_other, tap_other = note[0:ROWS], note[ROWS : ROWS + 1, 0:2]
    amat, bhi, blo, trans, refl = call(other_body, lookups(2), [SM] * 3 + [VM] * 6, flops=1 << 26)(
        tap_other, bank, media_table, map_other, *own
    )
    inc_cols = call(inc_column_body, [planes(33)], [VM] * 6, flops=1 << 26)(
        bhi, blo, incident, elow, ehigh, map_other
    )[0]
    utop, ubot = both_ways(inc_cols, inc_cols, "tx")
    strans, srefl = call(strips_body, [planes(2, 8)] * 2, [SM] + [VM] * 2, flops=1 << 25)(
        media_table, elow, ehigh
    )

    def two_ticks(first, outs, *args):
        scratch = [VM(*full(UNITS)), VM((2, 2, ROWS, COLS), f32), VM((2, 2, ROWS, COLS), f32)]
        return call(functools.partial(column_body, first), outs, [VM] * len(args), flops=1 << 27, scratch=scratch)(*args)

    mats = (bhi, blo, shi, slo, trans, refl, strans, srefl)
    x = two_ticks(True, [full(UNITS)], *mats, trans, w, low, high, hlow, hhigh)[0]
    htop, hbot = both_ways(x, x, "tx")
    wide = call(wide_body, [((2, 2, 128, 192), bf16)], [SM] * 3 + [pl.ANY], flops=1 << 24)(
        tap_index, tap_other, bank, x
    )[0]
    tall = ((8, 64, COLS), f32)
    tall_t, tall_r = call(taller_body, [tall] * 2, [SM] + [VM] * 4, flops=1 << 25)(
        media_table, trans, refl, utop, ubot
    )
    const = call(inc_row_body, [((UNITS, 2, 2, 64, COLS), f32)], [VM] * 5, flops=1 << 26)(
        wide, tall_t, inc_cols, utop, ubot
    )[0]
    w, low, high = call(second_body, [full(UNITS)] + [packs(3, UNITS)] * 2, [VM] * 7, flops=1 << 27)(
        amat, wide, tall_r, const, x, htop, hbot
    )
    hlow, hhigh = both_ways(low, high, "ty")
    top, bot = two_ticks(False, [half(UNITS)] * 2, *mats, const, w, low, high, hlow, hhigh)
    htop, hbot = both_ways(top, bot, "tx")
    down, up = call(
        last_body,
        [full(UNITS)] * 2,
        [VM] * 8,
        flops=1 << 27,
        scratch=[VM(*full(UNITS)), VM(*full(UNITS)), pltpu.SemaphoreType.DMA((UNITS,))],
        home=pl.ANY,
    )(
        amat, refl, const, incident, top, bot, htop, hbot
    )
    return down[None], up[None]


def solution(mesh):
    in_specs = (
        P("depth", None, None, None, "tx", "ty"),
        P("depth", None, None, None, "tx", "ty"),
        P(None, None, None, "tx", "ty"),
        P("depth", "tx", "ty"),
        P(),
        P("depth", None),
        P(),
    )
    out_specs = (P("depth", None, None, None, "tx", "ty"), P("depth", None, None, None, "tx", "ty"))
    return jax.shard_map(
        on_device, mesh=mesh, in_specs=in_specs, out_specs=out_specs, check_vma=False
    )
```
